32 devices in a mesh: row: 8 (over z, x), col: 4 (over y, core).
Axes of the slice: x: 2, y: 2, z: 4, core: 2. Of those that a mesh axis runs over, the one named last changes fastest.
Arguments:
- tensor: float32 [32, 1024, 1024], P(None, 'row', 'col'), may hold values from -6 to 6
- initial_first: float32 [1024, 256], P('row'), may hold values from -6 to 6
- initial_second: float32 [1024, 256], P('col'), may hold values from -6 to 6
Outputs:
- factor_first: float32 [1024, 256], P('row')
- factor_second: float32 [1024, 256], P('col')
- factor_frames: float32 [32, 256], replicated
- weights: float32 [256], replicated
The draws below stay inside these ranges and needn't reach their ends.
All inputs are finite; a program needn't handle non-finite values.
Results may differ from the reference program's by a relative error of at most 0.00024.
Values sent between devices are 32-bit elements; how exact they have to be, the bound alone decides.
A program may use at most 128 MiB of HBM per device.

```python
import math
import jax
import jax.numpy as jnp
from jax import lax

R = 256
K = 32
PASSES = 2
I = 1024
J = 1024


def block_scale(stream_key, shape, shards, least, high):
    factor_of = 1.0
    for position, parts in shards:
        draws = jax.random.uniform(jax.random.fold_in(jax.random.fold_in(stream_key, 6), position), (parts,), jnp.float32, least / len(shards), high / len(shards))
        factor_of = factor_of * jnp.repeat(jnp.exp(draws), shape[position] // parts).reshape((-1,) + (1,) * (len(shape) - 1 - position))
    return factor_of


def scatter_about(own_key, shape, scale, reach, split=(), dtype=jnp.bfloat16):
    array = jax.random.normal(own_key, shape, jnp.float32) * scale
    if len(split) > 0:
        array = block_scale(own_key, shape, split, -0.22, 0.18) * array
    return jnp.clip(array, min=-reach, max=reach).astype(dtype)


def setup_inputs(seed: int = 0) -> dict:
    seeds = jax.random.split(jax.random.key(seed), 4)
    return {
        "tensor": scatter_about(seeds[0], (K, I, J), 1.0, 6.0, ((1, 8), (2, 4)), jnp.float32),
        "initial_first": scatter_about(seeds[1], (I, R), 1.0, 6.0, ((0, 8),), jnp.float32),
        "initial_second": scatter_about(seeds[2], (J, R), 1.0, 6.0, ((0, 4),), jnp.float32),
    }


epsilon = 1e-06

def solve_gram(partials, hadamard):
    factor_lower = jnp.linalg.cholesky(hadamard)
    midway = lax.linalg.triangular_solve(factor_lower, partials, left_side=False, lower=True, transpose_a=True)
    return lax.linalg.triangular_solve(factor_lower, midway, left_side=False, lower=True, transpose_a=False)

def normalize(unscaled):
    scaling = jnp.sqrt(lax.optimization_barrier(jnp.mean(unscaled * unscaled, axis=0)) + epsilon)
    return (unscaled / scaling, scaling)

def gram_of(matrix):
    return jnp.dot(matrix.T, matrix, precision=lax.Precision.HIGHEST) / matrix.shape[0]

def reference(tensor, initial_first, initial_second):
    highest = lax.Precision.HIGHEST
    frames = tensor.shape[0]
    rows_first = tensor.shape[1]
    rows_second = tensor.shape[2]
    first_gram = gram_of(initial_first)
    second = initial_second
    second_gram = gram_of(initial_second)
    contracted = jnp.einsum('kij,ir->kjr', tensor, initial_first, precision=highest)
    for repeat in range(PASSES):
        frame_sums = jnp.einsum('kjr,jr->kr', contracted, second, precision=highest)
        frame_raw = solve_gram(frame_sums, first_gram * second_gram) / math.sqrt(rows_first * rows_second)
        factor_frames, unused = normalize(frame_raw)
        frame_gram = gram_of(factor_frames)
        second_sums = jnp.einsum('kjr,kr->jr', contracted, factor_frames, precision=highest)
        second_raw = solve_gram(second_sums, first_gram * frame_gram) / math.sqrt(rows_first * frames)
        second, unused = normalize(second_raw)
        second_gram = gram_of(second)
    second_contracted = jnp.einsum('kij,jr->kir', tensor, second, precision=highest)
    first_sums = jnp.einsum('kir,kr->ir', second_contracted, factor_frames, precision=highest)
    first_raw = solve_gram(first_sums, second_gram * frame_gram) / math.sqrt(rows_second * frames)
    factor_first, weights = normalize(first_raw)
    return (factor_first, second, factor_frames, weights)
```

```python
import functools
import math

import jax
import jax.numpy as jnp
from jax import lax
from jax.experimental import pallas as pl
from jax.experimental.pallas import tpu as pltpu
from jax.sharding import PartitionSpec as P

PASSES = 2
LANES = 128
PIVOTS = 8
MESH = pl.DeviceIdType.MESH
HIGHEST = lax.Precision.HIGHEST

epsilon = 1e-06


def product(a, b):
    return jnp.dot(a, b, precision=HIGHEST, preferred_element_type=jnp.float32)


def cross(a, b):
    return lax.dot_general(
        a, b, (((0,), (0,)), ((), ())), precision=HIGHEST, preferred_element_type=jnp.float32
    )


def invert(a, start, stop):
    size = a.shape[0]
    tiles = size // LANES
    row = lax.broadcasted_iota(jnp.int32, (PIVOTS, LANES), 0)
    lanes = [
        lax.broadcasted_iota(jnp.int32, (PIVOTS, LANES), 1) + q * LANES for q in range(tiles)
    ]
    wide = lax.broadcasted_iota(jnp.int32, (PIVOTS, size), 1)
    whole = lax.broadcasted_iota(jnp.int32, (size, size), 1)

    def step(g, carry):
        base = g * PIVOTS
        here = pl.ds(pl.multiple_of(base, PIVOTS), PIVOTS)
        rows = [a[here, q * LANES : (q + 1) * LANES] for q in range(tiles)]
        cols = []
        for t in range(PIVOTS):
            picked = sum(jnp.where(lanes[q] == base + t, rows[q], 0.0) for q in range(tiles))
            cols.append(
                jnp.broadcast_to(jnp.sum(picked, axis=1, keepdims=True), (PIVOTS, LANES))
            )
        work = []
        for q in range(tiles):
            place = lanes[q] - base
            inside = (place >= 0) & (place < PIVOTS)
            unit = jnp.where(place == row, 1.0, 0.0)
            work.append(jnp.where(inside, unit, rows[q]))
        for t in range(PIVOTS):
            pivot = 1.0 / jnp.broadcast_to(cols[t][t : t + 1, :], (PIVOTS, LANES))
            at = row == t

            def reduced(x):
                scaled = jnp.broadcast_to(x[t : t + 1, :], (PIVOTS, LANES)) * pivot
                return jnp.where(at, scaled, x - cols[t] * scaled)

            later = [reduced(cols[s]) for s in range(t + 1, PIVOTS)]
            work = [reduced(w) for w in work]
            cols[t + 1 :] = later
        solved = jnp.concatenate(work, axis=1)
        raw = a[here, :]
        inside = (wide >= base) & (wide < base + PIVOTS)
        left = jnp.where(inside, 0.0, jnp.where(wide < base, -raw, raw))
        kept = jnp.where((whole >= base) & (whole < base + PIVOTS), 0.0, a[...])
        a[...] = kept - cross(left, solved)
        a[here, :] = solved
        return carry

    lax.fori_loop(start, stop, step, 0)


def greet(sizes):
    barrier = pltpu.get_barrier_semaphore()
    for axis, n in sizes.items():
        me = lax.axis_index(axis)
        for d in range(1, n):
            pl.semaphore_signal(
                barrier, inc=1, device_id={axis: lax.rem(me + d, n)}, device_id_type=MESH
            )
    pl.semaphore_wait(barrier, sum(n - 1 for n in sizes.values()))


def scatter(axis, n, source, recv, sems):
    me = lax.axis_index(axis)
    chunk = recv.shape[1]
    copies = []
    for d in range(1, n):
        peer = lax.rem(me + d, n)
        copy = pltpu.make_async_remote_copy(
            src_ref=source.at[pl.ds(pl.multiple_of(peer * chunk, 8), chunk), :],
            dst_ref=recv.at[me],
            send_sem=sems.at[0, d - 1],
            recv_sem=sems.at[1, d - 1],
            device_id={axis: peer},
            device_id_type=MESH,
        )
        copy.start()
        copies.append(copy)
    recv[me] = source[pl.ds(pl.multiple_of(me * chunk, 8), chunk), :]
    return copies


def gather(axis, n, own, full, sems):
    me = lax.axis_index(axis)
    chunk = own.shape[0]
    place = pl.ds(pl.multiple_of(me * chunk, 8), chunk)
    full[place, :] = own
    copies = []
    for d in range(1, n):
        copy = pltpu.make_async_remote_copy(
            src_ref=full.at[place, :],
            dst_ref=full.at[place, :],
            send_sem=sems.at[0, d - 1],
            recv_sem=sems.at[1, d - 1],
            device_id={axis: lax.rem(me + d, n)},
            device_id_type=MESH,
        )
        copy.start()
        copies.append(copy)
    return copies


def finish(copies):
    for copy in copies:
        copy.wait()


def total(recv):
    result = recv[0]
    for s in range(1, recv.shape[0]):
        result = result + recv[s]
    return result


def total_blocks(full, n):
    chunk = full.shape[0] // n
    result = full[0:chunk, :]
    for s in range(1, n):
        result = result + full[s * chunk : (s + 1) * chunk, :]
    return result


def frames_of(sums, inverse, scale):
    raw = product(sums, inverse) * scale
    normed = raw / jnp.sqrt(jnp.mean(raw * raw, axis=0, keepdims=True) + epsilon)
    return normed, cross(normed, normed) / raw.shape[0]


def start_kernel(
    sizes, scales, gram1, gram2, terms, frames_out, frame_gram_out, first_gram_out,
    inv, recv1, recv2, full1, full2, parts1, parts2, s1, s2, s3, s4, s5, s6,
):
    row, col = sizes["row"], sizes["col"]
    greet(sizes)
    go1 = scatter("row", row, gram1, recv1, s1)
    go2 = scatter("col", col, gram2, recv2, s2)
    go3 = gather("row", row, terms[...], parts1, s3)
    finish(go2)
    go5 = gather("col", col, total(recv2), full2, s5)
    finish(go1)
    go4 = gather("row", row, total(recv1), full1, s4)
    finish(go3)
    go6 = gather("col", col, total_blocks(parts1, row), parts2, s6)
    finish(go4)
    finish(go5)
    first_gram = full1[...] * scales[0]
    first_gram_out[...] = first_gram
    inv[...] = first_gram * (full2[...] * scales[1])
    invert(inv, 0, inv.shape[0] // PIVOTS)
    finish(go6)
    normed, gram = frames_of(total_blocks(parts2, col), inv[...], scales[2])
    frames_out[...] = normed
    frame_gram_out[...] = gram


def frame_kernel(
    sizes, scales, first_gram, second_gram, terms, frames_out, frame_gram_out,
    inv, parts1, parts2, s1, s2,
):
    row, col = sizes["row"], sizes["col"]
    steps = inv.shape[0] // PIVOTS
    greet(sizes)
    go1 = gather("row", row, terms[...], parts1, s1)
    inv[...] = first_gram[...] * second_gram[...]
    invert(inv, 0, steps // 2)
    finish(go1)
    go2 = gather("col", col, total_blocks(parts1, row), parts2, s2)
    invert(inv, steps // 2, steps)
    finish(go2)
    normed, gram = frames_of(total_blocks(parts2, col), inv[...], scales[0])
    frames_out[...] = normed
    frame_gram_out[...] = gram


def second_kernel(
    sizes, scales, first_gram, frame_gram, terms, second_out, gram_out,
    inv, recv1, full1, local, recv2, full2, s1, s2, s3, s4,
):
    row, col = sizes["row"], sizes["col"]
    greet(sizes)
    go1 = scatter("row", row, terms, recv1, s1)
    inv[...] = first_gram[...] * frame_gram[...]
    invert(inv, 0, inv.shape[0] // PIVOTS)
    finish(go1)
    go2 = gather("row", row, product(total(recv1), inv[...]) * scales[0], full1, s2)
    finish(go2)
    raw = full1[...]
    local[...] = cross(raw, raw)
    go3 = scatter("col", col, local, recv2, s3)
    finish(go3)
    go4 = gather("col", col, total(recv2), full2, s4)
    finish(go4)
    gram = full2[...] * scales[1]
    size = gram.shape[0]
    down = lax.broadcasted_iota(jnp.int32, (size, size), 0)
    across = lax.broadcasted_iota(jnp.int32, (size, size), 1)
    diagonal = jnp.where(down == across, gram, 0.0)
    wide = jnp.sqrt(jnp.sum(diagonal, axis=0, keepdims=True) + epsilon)
    tall = jnp.sqrt(jnp.sum(diagonal, axis=1, keepdims=True) + epsilon)
    second_out[...] = raw / wide
    gram_out[...] = gram / wide / tall


def first_kernel(
    sizes, scales, second_gram, frame_gram, terms, first_out, weights_out,
    inv, recv1, full1, parts, s1, s2, s3,
):
    row, col = sizes["row"], sizes["col"]
    greet(sizes)
    go1 = scatter("col", col, terms, recv1, s1)
    inv[...] = second_gram[...] * frame_gram[...]
    invert(inv, 0, inv.shape[0] // PIVOTS)
    finish(go1)
    go2 = gather("col", col, product(total(recv1), inv[...]) * scales[0], full1, s2)
    finish(go2)
    raw = full1[...]
    squares = jnp.sum(raw * raw, axis=0, keepdims=True)
    go3 = gather("row", row, jnp.broadcast_to(squares, (8, raw.shape[1])), parts, s3)
    finish(go3)
    weights = jnp.sqrt(total_blocks(parts, row) * scales[1] + epsilon)
    weights_out[...] = weights
    first_out[...] = raw / weights[0:1, :]


def call(kernel, sizes, scales, args, outs, scratch, number, name):
    vmem = pl.BlockSpec(memory_space=pltpu.VMEM)
    return pl.pallas_call(
        functools.partial(kernel, sizes, scales),
        out_shape=[jax.ShapeDtypeStruct(shape, jnp.float32) for shape in outs],
        in_specs=[vmem] * len(args),
        out_specs=[vmem] * len(outs),
        scratch_shapes=scratch,
        compiler_params=pltpu.CompilerParams(
            collective_id=number, has_side_effects=True, vmem_limit_bytes=16 * 1024 * 1024
        ),
        name=name,
    )(*args)


def body(sizes, tensor, initial_first, initial_second):
    row, col = sizes["row"], sizes["col"]
    frames, own_first, own_second = tensor.shape
    rank = initial_first.shape[1]
    rows_first, rows_second = own_first * row, own_second * col
    square = (rank, rank)

    def vmem(*shape):
        return pltpu.VMEM(shape, jnp.float32)

    def sems(n):
        return pltpu.SemaphoreType.DMA((2, n - 1))

    def frame_terms(second):
        return jnp.einsum("kjr,jr->kr", contracted, second, precision=HIGHEST)

    gram1 = jnp.dot(initial_first.T, initial_first, precision=HIGHEST)
    gram2 = jnp.dot(initial_second.T, initial_second, precision=HIGHEST)
    contracted = jnp.einsum("kij,ir->kjr", tensor, initial_first, precision=HIGHEST)
    frame_scale = 1.0 / math.sqrt(rows_first * rows_second)
    second = initial_second
    for repeat in range(PASSES):
        terms = frame_terms(second)
        if repeat == 0:
            factor_frames, frame_gram, first_gram = call(
                start_kernel, sizes, (1.0 / rows_first, 1.0 / rows_second, frame_scale),
                (gram1, gram2, terms), ((frames, rank), square, square),
                [
                    vmem(*square), vmem(row, rank // row, rank), vmem(col, rank // col, rank),
                    vmem(*square), vmem(*square), vmem(row * frames, rank),
                    vmem(col * frames, rank),
                    sems(row), sems(col), sems(row), sems(row), sems(col), sems(col),
                ],
                0, "start",
            )
        else:
            factor_frames, frame_gram = call(
                frame_kernel, sizes, (frame_scale,), (first_gram, second_gram, terms),
                ((frames, rank), square),
                [
                    vmem(*square), vmem(row * frames, rank), vmem(col * frames, rank),
                    sems(row), sems(col),
                ],
                2 * repeat, "frame_%d" % repeat,
            )
        second_terms = jnp.einsum("kjr,kr->jr", contracted, factor_frames, precision=HIGHEST)
        second, second_gram = call(
            second_kernel, sizes, (1.0 / math.sqrt(rows_first * frames), 1.0 / rows_second),
            (first_gram, frame_gram, second_terms), ((own_second, rank), square),
            [
                vmem(*square), vmem(row, own_second // row, rank), vmem(own_second, rank),
                vmem(*square), vmem(col, rank // col, rank), vmem(*square),
                sems(row), sems(row), sems(col), sems(col),
            ],
            2 * repeat + 1, "second_%d" % repeat,
        )
    second_contracted = jnp.einsum("kij,jr->kir", tensor, second, precision=HIGHEST)
    first_terms = jnp.einsum("kir,kr->ir", second_contracted, factor_frames, precision=HIGHEST)
    factor_first, weights = call(
        first_kernel, sizes, (1.0 / math.sqrt(rows_second * frames), 1.0 / rows_first),
        (second_gram, frame_gram, first_terms), ((own_first, rank), (8, rank)),
        [
            vmem(*square), vmem(col, own_first // col, rank), vmem(own_first, rank),
            vmem(row * 8, rank), sems(col), sems(col), sems(row),
        ],
        2 * PASSES, "first",
    )
    return (factor_first, second, factor_frames, weights[0])


def solution(mesh):
    sizes = {"row": mesh.shape["row"], "col": mesh.shape["col"]}
    placed = (P(None, "row", "col"), P("row", None), P("col", None))
    return jax.shard_map(
        functools.partial(body, sizes),
        mesh=mesh,
        in_specs=placed,
        out_specs=(P("row", None), P("col", None), P(), P()),
        check_vma=False,
    )
```

```python
import functools
import math

import jax
import jax.numpy as jnp
from jax import lax
from jax.experimental import pallas as pl
from jax.experimental.pallas import tpu as pltpu
from jax.sharding import PartitionSpec as P

PASSES = 2
LANES = 128
PIVOTS = 16
MESH = pl.DeviceIdType.MESH
HIGHEST = lax.Precision.HIGHEST

epsilon = 1e-06


def product(a, b):
    return jnp.dot(a, b, precision=HIGHEST, preferred_element_type=jnp.float32)


def cross(a, b):
    return lax.dot_general(
        a, b, (((0,), (0,)), ((), ())), precision=HIGHEST, preferred_element_type=jnp.float32
    )


def invert(a, start, stop):
    size = a.shape[0]
    tiles = size // LANES
    row = lax.broadcasted_iota(jnp.int32, (PIVOTS, LANES), 0)
    lanes = [
        lax.broadcasted_iota(jnp.int32, (PIVOTS, LANES), 1) + q * LANES for q in range(tiles)
    ]
    wide = lax.broadcasted_iota(jnp.int32, (PIVOTS, size), 1)
    whole = lax.broadcasted_iota(jnp.int32, (size, size), 1)

    def step(g, carry):
        base = g * PIVOTS
        here = pl.ds(pl.multiple_of(base, PIVOTS), PIVOTS)
        rows = [a[here, q * LANES : (q + 1) * LANES] for q in range(tiles)]
        cols = []
        for t in range(PIVOTS):
            picked = sum(jnp.where(lanes[q] == base + t, rows[q], 0.0) for q in range(tiles))
            cols.append(
                jnp.broadcast_to(jnp.sum(picked, axis=1, keepdims=True), (PIVOTS, LANES))
            )
        work = []
        for q in range(tiles):
            place = lanes[q] - base
            inside = (place >= 0) & (place < PIVOTS)
            unit = jnp.where(place == row, 1.0, 0.0)
            work.append(jnp.where(inside, unit, rows[q]))
        for t in range(PIVOTS):
            pivot = 1.0 / jnp.broadcast_to(cols[t][t : t + 1, :], (PIVOTS, LANES))
            at = row == t

            def reduced(x):
                scaled = jnp.broadcast_to(x[t : t + 1, :], (PIVOTS, LANES)) * pivot
                return jnp.where(at, scaled, x - cols[t] * scaled)

            later = [reduced(cols[s]) for s in range(t + 1, PIVOTS)]
            work = [reduced(w) for w in work]
            cols[t + 1 :] = later
        solved = jnp.concatenate(work, axis=1)
        raw = a[here, :]
        inside = (wide >= base) & (wide < base + PIVOTS)
        left = jnp.where(inside, 0.0, jnp.where(wide < base, -raw, raw))
        kept = jnp.where((whole >= base) & (whole < base + PIVOTS), 0.0, a[...])
        a[...] = kept - cross(left, solved)
        a[here, :] = solved
        return carry

    lax.fori_loop(start, stop, step, 0)


def greet(sizes):
    barrier = pltpu.get_barrier_semaphore()
    for axis, n in sizes.items():
        me = lax.axis_index(axis)
        for d in range(1, n):
            pl.semaphore_signal(
                barrier, inc=1, device_id={axis: lax.rem(me + d, n)}, device_id_type=MESH
            )
    pl.semaphore_wait(barrier, sum(n - 1 for n in sizes.values()))


def scatter(axis, n, source, recv, sems):
    me = lax.axis_index(axis)
    chunk = recv.shape[1]
    copies = []
    for d in range(1, n):
        peer = lax.rem(me + d, n)
        copy = pltpu.make_async_remote_copy(
            src_ref=source.at[pl.ds(pl.multiple_of(peer * chunk, 8), chunk), :],
            dst_ref=recv.at[me],
            send_sem=sems.at[0, d - 1],
            recv_sem=sems.at[1, d - 1],
            device_id={axis: peer},
            device_id_type=MESH,
        )
        copy.start()
        copies.append(copy)
    recv[me] = source[pl.ds(pl.multiple_of(me * chunk, 8), chunk), :]
    return copies


def gather(axis, n, own, full, sems):
    me = lax.axis_index(axis)
    chunk = own.shape[0]
    place = pl.ds(pl.multiple_of(me * chunk, 8), chunk)
    full[place, :] = own
    copies = []
    for d in range(1, n):
        copy = pltpu.make_async_remote_copy(
            src_ref=full.at[place, :],
            dst_ref=full.at[place, :],
            send_sem=sems.at[0, d - 1],
            recv_sem=sems.at[1, d - 1],
            device_id={axis: lax.rem(me + d, n)},
            device_id_type=MESH,
        )
        copy.start()
        copies.append(copy)
    return copies


def finish(copies):
    for copy in copies:
        copy.wait()


def total(recv):
    result = recv[0]
    for s in range(1, recv.shape[0]):
        result = result + recv[s]
    return result


def total_blocks(full, n):
    chunk = full.shape[0] // n
    result = full[0:chunk, :]
    for s in range(1, n):
        result = result + full[s * chunk : (s + 1) * chunk, :]
    return result


def layout(sizes, frames, own_first, own_second, rank):
    row, col = sizes["row"], sizes["col"]
    square = (rank, rank)
    buffers = {
        "tens": (frames, own_first, own_second),
        "held": (frames, own_second, rank),
        "inv": square, "sums": (frames, rank),
        "gram_a": square, "recv_a": (row, rank // row, rank), "full_a": square,
        "gram_b": square, "recv_b": (col, rank // col, rank), "full_b": square,
        "terms_f": (own_first, rank), "recv_f": (col, own_first // col, rank),
        "raw_f": (own_first, rank), "parts_w": (row * 8, rank),
    }
    axes = {"a": row, "a2": row, "b": col, "b2": col, "f": col, "f2": col, "w": row}
    for p in range(PASSES):
        buffers.update({
            "parts_r%d" % p: (row * frames, rank), "parts_c%d" % p: (col * frames, rank),
            "terms_s%d" % p: (own_second, rank),
            "recv_s%d" % p: (row, own_second // row, rank), "raw_s%d" % p: (own_second, rank),
            "gram_g%d" % p: square, "recv_g%d" % p: (col, rank // col, rank),
            "full_g%d" % p: square,
        })
        axes.update({
            "r%d" % p: row, "c%d" % p: col, "s%d" % p: row, "t%d" % p: row,
            "g%d" % p: col, "h%d" % p: col,
        })
    names = list(buffers) + ["sem_" + name for name in axes] + ["sem_load"]
    shapes = [pltpu.VMEM(shape, jnp.float32) for shape in buffers.values()]
    shapes += [pltpu.SemaphoreType.DMA((2, n - 1)) for n in axes.values()]
    shapes += [pltpu.SemaphoreType.DMA((frames,))]
    return names, shapes


def kernel(sizes, names, tensor, first, second, first_out, second_out, frames_out, weights_out, *scratch):
    row, col = sizes["row"], sizes["col"]
    v = dict(zip(names, scratch))
    inv, sums, tens, held = v["inv"], v["sums"], v["tens"], v["held"]
    frames, own_first, own_second = tensor.shape
    rank = first.shape[1]
    rows_first, rows_second = own_first * row, own_second * col
    steps = rank // PIVOTS

    def load(k):
        return pltpu.make_async_copy(tensor.at[k], tens.at[k], v["sem_load"].at[k])

    def start_load(k, carry):
        load(k).start()
        return carry

    def contract(start, stop):
        def step(k, carry):
            load(k).wait()
            part = cross(tens[k], first[...])
            held[k] = part
            sums[pl.ds(k, 1), :] = jnp.sum(part * second[...], axis=0, keepdims=True)
            return carry

        lax.fori_loop(start, stop, step, 0)

    def frame_terms(raw):
        def step(k, carry):
            sums[pl.ds(k, 1), :] = jnp.sum(held[k] * raw[...], axis=0, keepdims=True)
            return carry

        lax.fori_loop(0, frames, step, 0)

    def second_terms(out):
        block = math.gcd(own_second, 64)
        for c in range(0, own_second, block):
            def step(k, total):
                return total + held[k, c : c + block, :] * frames_out[pl.ds(k, 1), :]

            out[c : c + block, :] = lax.fori_loop(
                0, frames, step, jnp.zeros((block, rank), jnp.float32), unroll=4
            )

    def first_terms(raw, start, stop):
        def step(k, carry):
            part = product(tens[k], raw[...])
            v["terms_f"][...] += part * frames_out[pl.ds(k, 1), :]
            return carry

        lax.fori_loop(start, stop, step, 0)

    def solve_frames(frame_sums):
        raw = product(frame_sums, inv[...]) * (1.0 / math.sqrt(rows_first * rows_second))
        normed = raw / jnp.sqrt(jnp.mean(raw * raw, axis=0, keepdims=True) + epsilon)
        frames_out[...] = normed
        return cross(normed, normed) / frames

    lax.fori_loop(0, frames, start_load, 0)
    v["gram_a"][...] = cross(first[...], first[...])
    v["gram_b"][...] = cross(second[...], second[...])
    greet(sizes)
    go_a = scatter("row", row, v["gram_a"], v["recv_a"], v["sem_a"])
    go_b = scatter("col", col, v["gram_b"], v["recv_b"], v["sem_b"])
    contract(0, frames // 2)
    finish(go_a)
    go_a = gather("row", row, total(v["recv_a"]), v["full_a"], v["sem_a2"])
    finish(go_b)
    go_b = gather("col", col, total(v["recv_b"]), v["full_b"], v["sem_b2"])
    contract(frames // 2, frames)
    finish(go_a)
    finish(go_b)
    first_gram = v["gram_a"]
    first_gram[...] = v["full_a"][...] * (1.0 / rows_first)
    second_gram = v["full_b"][...] * (1.0 / rows_second)
    wide = None
    for p in range(PASSES):
        here = str(p)
        if p == 0:
            go_r = gather("row", row, sums[...], v["parts_r0"], v["sem_r0"])
            inv[...] = first_gram[...] * second_gram
            invert(inv, 0, steps // 2)
            finish(go_r)
            go_c = gather(
                "col", col, total_blocks(v["parts_r0"], row), v["parts_c0"], v["sem_c0"]
            )
            invert(inv, steps // 2, steps)
        else:
            inv[...] = first_gram[...] * second_gram
            invert(inv, 0, steps)
        finish(go_c)
        frame_sums = total_blocks(v["parts_c" + here], col)
        if wide is not None:
            frame_sums = frame_sums / wide
        frame_gram = solve_frames(frame_sums)
        second_terms(v["terms_s" + here])
        go_s = scatter(
            "row", row, v["terms_s" + here], v["recv_s" + here], v["sem_s" + here]
        )
        inv[...] = first_gram[...] * frame_gram
        invert(inv, 0, steps)
        finish(go_s)
        solved = product(total(v["recv_s" + here]), inv[...])
        raw = v["raw_s" + here]
        go_s = gather(
            "row", row, solved * (1.0 / math.sqrt(rows_first * frames)), raw, v["sem_t" + here]
        )
        finish(go_s)
        v["gram_g" + here][...] = cross(raw[...], raw[...])
        go_g = scatter(
            "col", col, v["gram_g" + here], v["recv_g" + here], v["sem_g" + here]
        )
        last = p + 1 == PASSES
        if last:
            v["terms_f"][...] = jnp.zeros((own_first, rank), jnp.float32)
            first_terms(raw, 0, frames // 2)
        else:
            later = str(p + 1)
            frame_terms(raw)
            go_r = gather("row", row, sums[...], v["parts_r" + later], v["sem_r" + later])
        finish(go_g)
        go_g = gather(
            "col", col, total(v["recv_g" + here]), v["full_g" + here], v["sem_h" + here]
        )
        if last:
            first_terms(raw, frames // 2, frames)
            go_f = scatter("col", col, v["terms_f"], v["recv_f"], v["sem_f"])
        else:
            finish(go_r)
            go_c = gather(
                "col", col, total_blocks(v["parts_r" + later], row),
                v["parts_c" + later], v["sem_c" + later],
            )
        finish(go_g)
        gram = v["full_g" + here][...] * (1.0 / rows_second)
        down = lax.broadcasted_iota(jnp.int32, (rank, rank), 0)
        across = lax.broadcasted_iota(jnp.int32, (rank, rank), 1)
        diagonal = jnp.where(down == across, gram, 0.0)
        wide = jnp.sqrt(jnp.sum(diagonal, axis=0, keepdims=True) + epsilon)
        tall = jnp.sqrt(jnp.sum(diagonal, axis=1, keepdims=True) + epsilon)
        second_gram = gram / wide / tall
    inv[...] = second_gram * frame_gram
    second_out[...] = raw[...] / wide
    invert(inv, 0, steps)
    finish(go_f)
    solved = product(total(v["recv_f"]) / wide, inv[...])
    go_f = gather(
        "col", col, solved * (1.0 / math.sqrt(rows_second * frames)), v["raw_f"], v["sem_f2"]
    )
    finish(go_f)
    raw = v["raw_f"][...]
    squares = jnp.sum(raw * raw, axis=0, keepdims=True)
    go_w = gather("row", row, jnp.broadcast_to(squares, (8, rank)), v["parts_w"], v["sem_w"])
    finish(go_w)
    weights = jnp.sqrt(total_blocks(v["parts_w"], row) * (1.0 / rows_first) + epsilon)
    weights_out[...] = weights
    first_out[...] = raw / weights[0:1, :]


def body(sizes, tensor, initial_first, initial_second):
    frames, own_first, own_second = tensor.shape
    rank = initial_first.shape[1]
    names, scratch = layout(sizes, frames, own_first, own_second, rank)
    vmem = pl.BlockSpec(memory_space=pltpu.VMEM)
    outs = ((own_first, rank), (own_second, rank), (frames, rank), (8, rank))
    factor_first, second, factor_frames, weights = pl.pallas_call(
        functools.partial(kernel, sizes, names),
        out_shape=[jax.ShapeDtypeStruct(shape, jnp.float32) for shape in outs],
        in_specs=[pl.BlockSpec(memory_space=pl.ANY), vmem, vmem],
        out_specs=[vmem] * len(outs),
        scratch_shapes=scratch,
        compiler_params=pltpu.CompilerParams(
            collective_id=0, has_side_effects=True, vmem_limit_bytes=48 * 1024 * 1024
        ),
        name="als",
    )(tensor, initial_first, initial_second)
    return (factor_first, second, factor_frames, weights[0])


def solution(mesh):
    sizes = {"row": mesh.shape["row"], "col": mesh.shape["col"]}
    placed = (P(None, "row", "col"), P("row", None), P("col", None))
    return jax.shard_map(
        functools.partial(body, sizes),
        mesh=mesh,
        in_specs=placed,
        out_specs=(P("row", None), P("col", None), P(), P()),
        check_vma=False,
    )
```

```python
import functools
import math

import jax
import jax.numpy as jnp
from jax import lax
from jax.experimental import pallas as pl
from jax.experimental.pallas import tpu as pltpu
from jax.sharding import PartitionSpec as P

PASSES = 2
LANES = 128
PIVOTS = 16
MESH = pl.DeviceIdType.MESH
HIGHEST = lax.Precision.HIGHEST

epsilon = 1e-06


def product(a, b):
    return jnp.dot(a, b, precision=HIGHEST, preferred_element_type=jnp.float32)


def cross(a, b):
    return lax.dot_general(
        a, b, (((0,), (0,)), ((), ())), precision=HIGHEST, preferred_element_type=jnp.float32
    )


def invert(a, start, stop):
    size = a.shape[0]
    tiles = size // LANES
    row = lax.broadcasted_iota(jnp.int32, (PIVOTS, LANES), 0)
    lanes = [
        lax.broadcasted_iota(jnp.int32, (PIVOTS, LANES), 1) + q * LANES for q in range(tiles)
    ]
    wide = lax.broadcasted_iota(jnp.int32, (PIVOTS, size), 1)
    whole = lax.broadcasted_iota(jnp.int32, (size, size), 1)

    def step(g, carry):
        base = g * PIVOTS
        here = pl.ds(pl.multiple_of(base, PIVOTS), PIVOTS)
        rows = [a[here, q * LANES : (q + 1) * LANES] for q in range(tiles)]
        cols = []
        for t in range(PIVOTS):
            picked = sum(jnp.where(lanes[q] == base + t, rows[q], 0.0) for q in range(tiles))
            cols.append(
                jnp.broadcast_to(jnp.sum(picked, axis=1, keepdims=True), (PIVOTS, LANES))
            )
        work = []
        for q in range(tiles):
            place = lanes[q] - base
            inside = (place >= 0) & (place < PIVOTS)
            unit = jnp.where(place == row, 1.0, 0.0)
            work.append(jnp.where(inside, unit, rows[q]))
        for t in range(PIVOTS):
            pivot = 1.0 / jnp.broadcast_to(cols[t][t : t + 1, :], (PIVOTS, LANES))
            at = row == t

            def reduced(x):
                scaled = jnp.broadcast_to(x[t : t + 1, :], (PIVOTS, LANES)) * pivot
                return jnp.where(at, scaled, x - cols[t] * scaled)

            later = [reduced(cols[s]) for s in range(t + 1, PIVOTS)]
            work = [reduced(w) for w in work]
            cols[t + 1 :] = later
        solved = jnp.concatenate(work, axis=1)
        raw = a[here, :]
        inside = (wide >= base) & (wide < base + PIVOTS)
        left = jnp.where(inside, 0.0, jnp.where(wide < base, -raw, raw))
        kept = jnp.where((whole >= base) & (whole < base + PIVOTS), 0.0, a[...])
        a[...] = kept - cross(left, solved)
        a[here, :] = solved
        return carry

    lax.fori_loop(start, stop, step, 0)


def greet(sizes):
    barrier = pltpu.get_barrier_semaphore()
    for axis, n in sizes.items():
        me = lax.axis_index(axis)
        for d in range(1, n):
            pl.semaphore_signal(
                barrier, inc=1, device_id={axis: lax.rem(me + d, n)}, device_id_type=MESH
            )
    pl.semaphore_wait(barrier, sum(n - 1 for n in sizes.values()))


def scatter(axis, n, source, recv, sems):
    me = lax.axis_index(axis)
    chunk = recv.shape[1]
    copies = []
    for d in range(1, n):
        peer = lax.rem(me + d, n)
        copy = pltpu.make_async_remote_copy(
            src_ref=source.at[pl.ds(pl.multiple_of(peer * chunk, 8), chunk), :],
            dst_ref=recv.at[me],
            send_sem=sems.at[0, d - 1],
            recv_sem=sems.at[1, d - 1],
            device_id={axis: peer},
            device_id_type=MESH,
        )
        copy.start()
        copies.append(copy)
    recv[me] = source[pl.ds(pl.multiple_of(me * chunk, 8), chunk), :]
    return copies


def gather(axis, n, own, full, sems):
    me = lax.axis_index(axis)
    chunk = own.shape[0]
    place = pl.ds(pl.multiple_of(me * chunk, 8), chunk)
    full[place, :] = own
    copies = []
    for d in range(1, n):
        copy = pltpu.make_async_remote_copy(
            src_ref=full.at[place, :],
            dst_ref=full.at[place, :],
            send_sem=sems.at[0, d - 1],
            recv_sem=sems.at[1, d - 1],
            device_id={axis: lax.rem(me + d, n)},
            device_id_type=MESH,
        )
        copy.start()
        copies.append(copy)
    return copies


def finish(copies):
    for copy in copies:
        copy.wait()


def total(recv):
    result = recv[0]
    for s in range(1, recv.shape[0]):
        result = result + recv[s]
    return result


def total_blocks(full, n):
    chunk = full.shape[0] // n
    result = full[0:chunk, :]
    for s in range(1, n):
        result = result + full[s * chunk : (s + 1) * chunk, :]
    return result


def layout(sizes, frames, own_first, own_second, rank):
    row, col = sizes["row"], sizes["col"]
    square = (rank, rank)
    buffers = {
        "tens": (frames, own_first, own_second),
        "held": (frames, own_second, rank),
        "inv": square, "sums": (frames, rank),
        "gram_a": square, "recv_a": (row, rank // row, rank), "full_a": square,
        "gram_b": square, "recv_b": (col, rank // col, rank), "full_b": square,
        "terms_f": (own_first, rank), "recv_f": (col, own_first // col, rank),
        "raw_f": (own_first, rank), "parts_w": (row * 8, rank),
    }
    axes = {"a": row, "a2": row, "b": col, "b2": col, "f": col, "f2": col, "w": row}
    for p in range(PASSES):
        buffers.update({
            "parts_r%d" % p: (row * frames, rank), "parts_c%d" % p: (col * frames, rank),
            "terms_s%d" % p: (own_second, rank),
            "recv_s%d" % p: (row, own_second // row, rank), "raw_s%d" % p: (own_second, rank),
            "gram_g%d" % p: square, "recv_g%d" % p: (col, rank // col, rank),
            "full_g%d" % p: square,
        })
        axes.update({
            "r%d" % p: row, "c%d" % p: col, "s%d" % p: row, "t%d" % p: row,
            "g%d" % p: col, "h%d" % p: col,
        })
    names = list(buffers) + ["sem_" + name for name in axes] + ["sem_load"]
    shapes = [pltpu.VMEM(shape, jnp.float32) for shape in buffers.values()]
    shapes += [pltpu.SemaphoreType.DMA((2, n - 1)) for n in axes.values()]
    shapes += [pltpu.SemaphoreType.DMA((frames,))]
    return names, shapes


def kernel(sizes, names, tensor, first, second, first_out, second_out, frames_out, weights_out, *scratch):
    row, col = sizes["row"], sizes["col"]
    v = dict(zip(names, scratch))
    inv, sums, tens, held = v["inv"], v["sums"], v["tens"], v["held"]
    frames, own_first, own_second = tensor.shape
    rank = first.shape[1]
    rows_first, rows_second = own_first * row, own_second * col
    steps = rank // PIVOTS

    def load(k):
        return pltpu.make_async_copy(tensor.at[k], tens.at[k], v["sem_load"].at[k])

    def start_load(k, carry):
        load(k).start()
        return carry

    def contract(start, stop):
        group = math.gcd(stop - start, 4)

        def step(g, carry):
            ks = [start + g * group + u for u in range(group)]
            for k in ks:
                load(k).wait()
            parts = [cross(tens[k], first[...]) for k in ks]
            for k, part in zip(ks, parts):
                held[k] = part
                sums[pl.ds(k, 1), :] = jnp.sum(part * second[...], axis=0, keepdims=True)
            return carry

        lax.fori_loop(0, (stop - start) // group, step, 0)

    def frame_terms(raw):
        def step(k, carry):
            sums[pl.ds(k, 1), :] = jnp.sum(held[k] * raw[...], axis=0, keepdims=True)
            return carry

        lax.fori_loop(0, frames, step, 0)

    def second_terms(out):
        block = math.gcd(own_second, 64)
        for c in range(0, own_second, block):
            def step(k, total):
                return total + held[k, c : c + block, :] * frames_out[pl.ds(k, 1), :]

            out[c : c + block, :] = lax.fori_loop(
                0, frames, step, jnp.zeros((block, rank), jnp.float32), unroll=4
            )

    def first_terms(raw, start, stop):
        group = math.gcd(stop - start, 4)

        def step(g, carry):
            base = start + g * group
            stacked = tens[pl.ds(base, group)].reshape(group * own_first, own_second)
            part = product(stacked, raw[...])
            v["terms_f"][...] += sum(
                part[u * own_first : (u + 1) * own_first, :] * frames_out[pl.ds(base + u, 1), :]
                for u in range(group)
            )
            return carry

        lax.fori_loop(0, (stop - start) // group, step, 0)

    def solve_frames(frame_sums):
        raw = product(frame_sums, inv[...]) * (1.0 / math.sqrt(rows_first * rows_second))
        normed = raw / jnp.sqrt(jnp.mean(raw * raw, axis=0, keepdims=True) + epsilon)
        frames_out[...] = normed
        return cross(normed, normed) / frames

    lax.fori_loop(0, frames, start_load, 0)
    v["gram_a"][...] = cross(first[...], first[...])
    v["gram_b"][...] = cross(second[...], second[...])
    greet(sizes)
    go_a = scatter("row", row, v["gram_a"], v["recv_a"], v["sem_a"])
    go_b = scatter("col", col, v["gram_b"], v["recv_b"], v["sem_b"])
    contract(0, frames // 2)
    finish(go_a)
    go_a = gather("row", row, total(v["recv_a"]), v["full_a"], v["sem_a2"])
    finish(go_b)
    go_b = gather("col", col, total(v["recv_b"]), v["full_b"], v["sem_b2"])
    contract(frames // 2, frames)
    finish(go_a)
    finish(go_b)
    first_gram = v["gram_a"]
    first_gram[...] = v["full_a"][...] * (1.0 / rows_first)
    second_gram = v["full_b"][...] * (1.0 / rows_second)
    wide = None
    for p in range(PASSES):
        here = str(p)
        if p == 0:
            go_r = gather("row", row, sums[...], v["parts_r0"], v["sem_r0"])
            inv[...] = first_gram[...] * second_gram
            invert(inv, 0, steps // 2)
            finish(go_r)
            go_c = gather(
                "col", col, total_blocks(v["parts_r0"], row), v["parts_c0"], v["sem_c0"]
            )
            invert(inv, steps // 2, steps)
        else:
            inv[...] = first_gram[...] * second_gram
            invert(inv, 0, steps)
        finish(go_c)
        frame_sums = total_blocks(v["parts_c" + here], col)
        if wide is not None:
            frame_sums = frame_sums / wide
        frame_gram = solve_frames(frame_sums)
        second_terms(v["terms_s" + here])
        go_s = scatter(
            "row", row, v["terms_s" + here], v["recv_s" + here], v["sem_s" + here]
        )
        inv[...] = first_gram[...] * frame_gram
        invert(inv, 0, steps)
        finish(go_s)
        solved = product(total(v["recv_s" + here]), inv[...])
        raw = v["raw_s" + here]
        go_s = gather(
            "row", row, solved * (1.0 / math.sqrt(rows_first * frames)), raw, v["sem_t" + here]
        )
        finish(go_s)
        v["gram_g" + here][...] = cross(raw[...], raw[...])
        go_g = scatter(
            "col", col, v["gram_g" + here], v["recv_g" + here], v["sem_g" + here]
        )
        last = p + 1 == PASSES
        if last:
            v["terms_f"][...] = jnp.zeros((own_first, rank), jnp.float32)
            first_terms(raw, 0, frames // 2)
        else:
            later = str(p + 1)
            frame_terms(raw)
            go_r = gather("row", row, sums[...], v["parts_r" + later], v["sem_r" + later])
        finish(go_g)
        go_g = gather(
            "col", col, total(v["recv_g" + here]), v["full_g" + here], v["sem_h" + here]
        )
        if last:
            first_terms(raw, frames // 2, frames)
            go_f = scatter("col", col, v["terms_f"], v["recv_f"], v["sem_f"])
        else:
            finish(go_r)
            go_c = gather(
                "col", col, total_blocks(v["parts_r" + later], row),
                v["parts_c" + later], v["sem_c" + later],
            )
        finish(go_g)
        gram = v["full_g" + here][...] * (1.0 / rows_second)
        down = lax.broadcasted_iota(jnp.int32, (rank, rank), 0)
        across = lax.broadcasted_iota(jnp.int32, (rank, rank), 1)
        diagonal = jnp.where(down == across, gram, 0.0)
        wide = jnp.sqrt(jnp.sum(diagonal, axis=0, keepdims=True) + epsilon)
        tall = jnp.sqrt(jnp.sum(diagonal, axis=1, keepdims=True) + epsilon)
        second_gram = gram / wide / tall
    inv[...] = second_gram * frame_gram
    second_out[...] = raw[...] / wide
    invert(inv, 0, steps)
    finish(go_f)
    solved = product(total(v["recv_f"]) / wide, inv[...])
    go_f = gather(
        "col", col, solved * (1.0 / math.sqrt(rows_second * frames)), v["raw_f"], v["sem_f2"]
    )
    finish(go_f)
    raw = v["raw_f"][...]
    squares = jnp.sum(raw * raw, axis=0, keepdims=True)
    go_w = gather("row", row, jnp.broadcast_to(squares, (8, rank)), v["parts_w"], v["sem_w"])
    finish(go_w)
    weights = jnp.sqrt(total_blocks(v["parts_w"], row) * (1.0 / rows_first) + epsilon)
    weights_out[...] = weights
    first_out[...] = raw / weights[0:1, :]


def body(sizes, tensor, initial_first, initial_second):
    frames, own_first, own_second = tensor.shape
    rank = initial_first.shape[1]
    names, scratch = layout(sizes, frames, own_first, own_second, rank)
    vmem = pl.BlockSpec(memory_space=pltpu.VMEM)
    outs = ((own_first, rank), (own_second, rank), (frames, rank), (8, rank))
    factor_first, second, factor_frames, weights = pl.pallas_call(
        functools.partial(kernel, sizes, names),
        out_shape=[jax.ShapeDtypeStruct(shape, jnp.float32) for shape in outs],
        in_specs=[pl.BlockSpec(memory_space=pl.ANY), vmem, vmem],
        out_specs=[vmem] * len(outs),
        scratch_shapes=scratch,
        compiler_params=pltpu.CompilerParams(
            collective_id=0, has_side_effects=True, vmem_limit_bytes=48 * 1024 * 1024
        ),
        name="als",
    )(tensor, initial_first, initial_second)
    return (factor_first, second, factor_frames, weights[0])


def solution(mesh):
    sizes = {"row": mesh.shape["row"], "col": mesh.shape["col"]}
    placed = (P(None, "row", "col"), P("row", None), P("col", None))
    return jax.shard_map(
        functools.partial(body, sizes),
        mesh=mesh,
        in_specs=placed,
        out_specs=(P("row", None), P("col", None), P(), P()),
        check_vma=False,
    )
```
